32 devices in a mesh: space: 32 (over z, y, x, core), ens: 1.
Axes of the slice: x: 2, y: 2, z: 4, core: 2. Of those that a mesh axis runs over, the one named last changes fastest.
Arguments:
- innovations: bfloat16 [1, 2048, 128, 128], P('ens', 'space'), may hold values from -6 to 6
- block_owner: int32 [2048, 1], P('space'), may hold values from 0 to 31; in each aligned block of 64 rows (0 to 63, 64 to 127, ...) at most 4 rows name the same one
- block_tile: int32 [2048], P('space'), may hold values from 0 to 3
- block_count: int32 [32], P('space'), may hold values from 48 to 64
- obs_row: int32 [2048, 128], P('space'), may hold values from 0 to 6
- obs_col: int32 [2048, 128], P('space'), may hold values from 0 to 14
- offsets: float32 [2048, 2, 128], P('space'), may hold values from 0 to 1
- obs_mask: int32 [2048, 128], P('space'), may hold values 0 or 1
- sigma: float32 [128, 128], P('space'), may hold values from 0.3 to 3
- coupling: float32 [128, 128], replicated, may hold values from -0.5 to 0.5
Outputs:
- gradient: float32 [128, 128, 128], P('ens', 'space')
The draws below stay inside these ranges and needn't reach their ends.
Inputs may be any that keep to these rules, and one draw needn't show every extreme that they name: `block_owner`: among the rows of one device, no owner is named more than 4 times, and one owner is named exactly 4 times in some devices' rows. `block_count`: blocks of a device at positions at or above its count are padding.
All inputs are finite; a program needn't handle non-finite values. No bound on the sum of `obs_mask` on one device may be relied on, other than what follows from the above.
Results may differ from the reference program's by a relative error of at most 0.0095.
Values may be sent and summed in bfloat16 or wider, within the bound.
No kernel may reach another device: no remote copies, remote signals or barrier semaphores. Data moves between devices by JAX's collectives and lax.ppermute only.
A program may use at most 64 MiB of HBM per device.

```python
import math
import jax
import jax.numpy as jnp
import numpy as np
from jax import lax

CH = 128
OBS = 128
TH = 8
TW = 16
CELLS = 128
TILE_DEV = 4
TILES = 128
BLK_DEV = 64
BLOCKS = 2048
CAP = 4
MEMBERS = 1
N_SPACE = 32


def with_ends(array, own_key, low, largest):
    place = [jax.random.randint(jax.random.fold_in(own_key, axis), (), 0, length) for axis, length in enumerate(array.shape)]
    main_axis = array.shape.index(max(array.shape))
    beside = place[:main_axis] + [(place[main_axis] + 1) % array.shape[main_axis]] + place[main_axis + 1:]
    return array.at[tuple(place)].set(low).at[tuple(beside)].set(largest)


def levels(own_key, shape, pieces, least, high):
    def one(dim, blocks):
        draws = jax.random.uniform(jax.random.fold_in(jax.random.fold_in(own_key, 6), dim), (blocks,), jnp.float32, least / len(pieces), high / len(pieces))
        return jnp.repeat(jnp.exp(draws), shape[dim] // blocks).reshape((-1,) + (1,) * (len(shape) - dim - 1))

    loudness = one(*pieces[0])
    for cut in pieces[1:]:
        loudness = loudness * one(*cut)
    return loudness


def routed_block(stream_key, own, number, rows, amount, top, reach, skew):
    order = jax.random.permutation(stream_key, amount)
    crowded, common = shares(amount, rows * top, reach, skew, True), shares(amount, rows * top, reach, skew, False)
    places = jnp.arange(amount)

    def named(sizes, rotation):
        used = int((sizes > 0).sum())
        fixed = max(1, used // 4)
        shifted = fixed + (places - fixed + rotation * (used - fixed)) % max(1, amount - fixed)
        return jnp.zeros((amount,), jnp.int32).at[order[jnp.where(places < fixed, places, shifted)]].set(jnp.asarray(sizes, jnp.int32))

    sizes = jnp.where(number % 4 == 0, named(crowded, number // 4), named(common, number - number // 4 - 1))
    mixed = jax.random.permutation(jax.random.fold_in(own, 3), amount)
    donor, taker = mixed[0:amount // 2 * 2:2], mixed[1:amount // 2 * 2:2]
    margin = jnp.minimum(sizes[donor] - 1, reach - sizes[taker]) // 2
    margin = jnp.where((donor == order[0]) | (taker == order[0]) | (sizes[taker] == 0), 0, jnp.maximum(margin, 0))
    shifted = jax.random.randint(jax.random.fold_in(own, 4), (amount // 2,), 0, 1 << 20) % (margin + 1)
    sizes = sizes.at[donor].add(-shifted).at[taker].add(shifted)
    labels = jnp.searchsorted(jnp.cumsum(sizes), jnp.arange(rows * top), side="right").astype(jnp.int32)
    grid = labels.reshape(top, rows).T
    grid = grid[jax.random.permutation(jax.random.fold_in(own, 1), rows)]
    rotation = jax.random.randint(jax.random.fold_in(own, 2), (rows, 1), 0, top)
    return jnp.take_along_axis(grid, (jnp.arange(top)[None, :] + rotation) % top, axis=1)


def shares(amount, total, bound, lean, full):
    loads = [(1 << 20) // math.isqrt(rank ** lean) + 1 for rank in range(1, amount + 1)]
    largest = bound if full else min(bound, max(-(-total // amount), total * loads[0] // sum(loads)))
    least = 1 if total - largest >= amount - 1 else 0
    holding, rest = [largest] + [least] * (amount - 1), total - largest - least * (amount - 1)
    while rest > 0:
        free = [i for i in range(1, amount) if holding[i] < largest] or [i for i in range(1, amount) if holding[i] < bound]
        pool, remaining = sum([loads[i] for i in free]), rest
        for i in free:
            extra = min(bound - holding[i], max(1, remaining * loads[i] // pool), rest)
            holding[i] = holding[i] + extra
            rest = rest - extra
    return np.array(holding)


def noise(own_key, extent, width, bound, cuts=(), kind=jnp.bfloat16):
    array = jax.random.normal(own_key, extent, jnp.float32) * width
    if len(cuts) > 0:
        array = levels(own_key, extent, cuts, -0.22, 0.18) * array
    return jnp.clip(array, min=-bound, max=bound).astype(kind)


def setup_inputs(seed: int = 0) -> dict:
    keys = jax.random.split(jax.random.key(seed), 11)
    innovations = noise(keys[0], (MEMBERS, BLOCKS, OBS, CH), 1.0, 6.0, ((1, 32),))
    block_owner_keys = jax.random.split(jax.random.fold_in(keys[1], 1), BLOCKS // BLK_DEV)
    block_owner_turns = jax.random.permutation(jax.random.fold_in(keys[1], 3), BLOCKS // BLK_DEV)
    block_owner = jax.vmap(lambda own, number: routed_block(jax.random.fold_in(keys[1], 2), own, number, BLK_DEV, N_SPACE, 1, CAP, 2))(block_owner_keys, block_owner_turns).reshape((BLOCKS, 1))
    block_tile = with_ends(jax.random.randint(keys[2], (BLOCKS,), 0, TILE_DEV), jax.random.fold_in(keys[2], 1), 0, TILE_DEV - 1).astype(jnp.int32)
    block_count = with_ends(jax.random.randint(keys[3], (N_SPACE,), 3 * BLK_DEV // 4, BLK_DEV + 1), jax.random.fold_in(keys[3], 1), 3 * BLK_DEV // 4, BLK_DEV).astype(jnp.int32)
    obs_row = with_ends(jax.random.randint(keys[4], (BLOCKS, OBS), 0, TH - 1), jax.random.fold_in(keys[4], 1), 0, (TH - 1) - 1).astype(jnp.int32)
    obs_col = with_ends(jax.random.randint(keys[5], (BLOCKS, OBS), 0, TW - 1), jax.random.fold_in(keys[5], 1), 0, (TW - 1) - 1).astype(jnp.int32)
    offsets = jnp.clip(1.0 * jax.random.uniform(keys[6], (BLOCKS, 2, OBS), jnp.float32) ** levels(keys[6], (BLOCKS, 2, OBS), ((0, 32),), -0.2, 0.2), 0.0, 1.0)
    obs_mask = with_ends((jax.random.randint(keys[7], (BLOCKS, OBS), 0, 4) < 3).astype(jnp.int32), jax.random.fold_in(keys[7], 1), 0, 1)
    sigma = jnp.clip(jnp.exp(math.log(3.0) - 2.3025851 * jax.random.uniform(keys[8], (TILES, CH), jnp.float32) ** levels(keys[8], (TILES, CH), ((0, 32),), -0.2, 0.2)), 0.3, 3.0)
    coupling = noise(keys[9], (CELLS, CELLS), CELLS ** -0.5, 0.5, (), jnp.float32)
    return {"innovations": innovations, "block_owner": block_owner, "block_tile": block_tile, "block_count": block_count, "obs_row": obs_row, "obs_col": obs_col, "offsets": offsets, "obs_mask": obs_mask, "sigma": sigma, "coupling": coupling}


def reference(innovations, block_owner, block_tile, block_count, obs_row, obs_col, offsets, obs_mask, sigma, coupling):
    blocks = block_owner.shape[0]
    per_device = blocks // block_count.shape[0]
    position = jnp.arange(blocks, dtype=jnp.int32)
    alive = (position % per_device) < block_count[position // per_device]
    live = obs_mask.astype(jnp.float32) * alive[:, None].astype(jnp.float32)
    row_frac = offsets[:, 0, :]
    col_frac = offsets[:, 1, :]
    tile = block_owner[:, 0] * TILE_DEV + block_tile
    summed = jnp.sum(innovations.astype(jnp.float32), axis=0).reshape(-1, CH)
    total = jnp.zeros((TILES * CELLS, CH), jnp.float32)
    for down in (0, 1):
        for right in (0, 1):
            row_part = row_frac if down == 1 else 1.0 - row_frac
            col_part = col_frac if right == 1 else 1.0 - col_frac
            rounded = (row_part * col_part * live).astype(jnp.bfloat16)
            rounded = lax.optimization_barrier(rounded).astype(jnp.float32)
            target = tile[:, None] * CELLS + (obs_row + down) * TW + obs_col + right
            total = total.at[target.reshape(-1)].add(summed * rounded.reshape(-1, 1))
    mean = total.reshape(TILES, CELLS, CH) / MEMBERS
    coupled = jnp.einsum("ck,tkh->cth", coupling, mean, precision=lax.Precision.HIGHEST)
    return sigma[None, :, :] * (jnp.transpose(mean, (1, 0, 2)) + coupled)
```

```python
import functools

import jax
import jax.numpy as jnp
from jax import lax
from jax.experimental import pallas as pl
from jax.experimental.pallas import tpu as pltpu
from jax.sharding import PartitionSpec as P

TW = 16


def scaled_rows(totals, coupling, sigma, start, count, members):
    coupling_rows = lax.dynamic_slice_in_dim(coupling, start, count, 0)
    own = lax.dynamic_slice_in_dim(totals, start, count, 1)
    coupled = jnp.einsum("ck,tkh->cth", coupling_rows, totals, precision=lax.Precision.HIGHEST)
    return sigma[None, :, :] * (jnp.transpose(own, (1, 0, 2)) + coupled) / members


def stage_orders(bits):
    first = list(range(bits))
    second = list(first)
    if bits > 2:
        second[1], second[2] = second[2], second[1]
    return first, second


def scatter_kernel(
    owner_ref,
    tile_ref,
    count_ref,
    row_ref,
    col_ref,
    offsets_ref,
    mask_ref,
    values_ref,
    *refs,
    orders,
    tile_local,
    unroll,
):
    streams = len(orders)
    keeps, sends, accs = refs[:streams], refs[streams : 2 * streams], refs[2 * streams :]
    blk_local, obs_count, width = values_ref.shape
    part = accs[0].shape[1]
    rows = streams * part // TW
    me = lax.axis_index("space")
    for acc in accs:
        acc[...] = jnp.zeros(acc.shape, acc.dtype)
    row_ids = lax.broadcasted_iota(jnp.int32, (rows, obs_count), 0)
    col_ids = lax.broadcasted_iota(jnp.int32, (TW, obs_count), 0)

    def one(block):
        relative = jnp.bitwise_xor(owner_ref[block], me)
        row = row_ref[pl.ds(block, 1), :]
        col = col_ref[pl.ds(block, 1), :]
        row_frac = offsets_ref[block, 0:1, :]
        col_frac = offsets_ref[block, 1:2, :]
        alive = jnp.where(block < count_ref[0], 1.0, 0.0)
        live = mask_ref[pl.ds(block, 1), :].astype(jnp.float32) * alive
        row_off = row_ids - row
        row_part = jnp.where(
            row_off == 0,
            (1.0 - row_frac) * live,
            jnp.where(row_off == 1, row_frac * live, 0.0),
        )
        col_off = col_ids - col
        col_part = jnp.where(
            col_off == 0, 1.0 - col_frac, jnp.where(col_off == 1, col_frac, 0.0)
        )
        table = (row_part[:, None, :] * col_part[None, :, :]).reshape(rows * TW, obs_count)
        contrib = jnp.dot(
            table.astype(jnp.bfloat16), values_ref[block], preferred_element_type=jnp.float32
        )
        for index, (order, acc) in enumerate(zip(orders, accs)):
            place = jnp.int32(0)
            for bit in order:
                place = place * 2 + (lax.shift_right_logical(relative, bit) & 1)
            slot = place * tile_local + tile_ref[block]
            acc[slot] += contrib[index * part : (index + 1) * part]

    def several(turn, carry):
        for step in range(unroll):
            one(turn * unroll + step)
        return carry

    lax.fori_loop(0, blk_local // unroll, several, 0)
    for keep, send, acc in zip(keeps, sends, accs):
        half = keep.shape[0]

        def convert(slot, carry, keep=keep, send=send, acc=acc, half=half):
            for step in range(tile_local):
                at = slot * tile_local + step
                keep[at] = acc[at].astype(keep.dtype)
                send[at] = acc[half + at].astype(send.dtype)
            return carry

        lax.fori_loop(0, half // tile_local, convert, 0)


def scatter_blocks(
    owner, block_tile, block_count, row, col, offsets, mask, values, orders, tile_local, cells
):
    streams = len(orders)
    slots = 2 ** len(orders[0]) * tile_local
    part = cells // streams
    width = values.shape[2]
    blk_local = values.shape[0]
    unroll = 4 if blk_local % 4 == 0 else 1
    half = jax.ShapeDtypeStruct((slots // 2, part, width), jnp.bfloat16)
    in_smem = pl.BlockSpec(memory_space=pltpu.SMEM)
    in_vmem = pl.BlockSpec(memory_space=pltpu.VMEM)
    return pl.pallas_call(
        functools.partial(scatter_kernel, orders=orders, tile_local=tile_local, unroll=unroll),
        in_specs=[in_smem] * 3 + [in_vmem] * 5,
        out_specs=[in_vmem] * (2 * streams),
        out_shape=[half] * (2 * streams),
        scratch_shapes=[pltpu.VMEM((slots, part, width), jnp.float32)] * streams,
        compiler_params=pltpu.CompilerParams(vmem_limit_bytes=60 * 1024 * 1024),
    )(owner, block_tile, block_count, row, col, offsets, mask, values)


def exchange(part, bit, peers):
    return lax.ppermute(part, "space", [(i, i ^ (1 << bit)) for i in range(peers)])


def added(kept, got):
    return kept.astype(jnp.float32) + got.astype(jnp.float32)


def on_device(
    innovations,
    block_owner,
    block_tile,
    block_count,
    obs_row,
    obs_col,
    offsets,
    obs_mask,
    sigma,
    coupling,
):
    peers = lax.axis_size("space")
    tile_local = sigma.shape[0]
    cell_count = coupling.shape[0]
    ens_count = lax.axis_size("ens")
    members = ens_count * innovations.shape[0]
    share = cell_count // ens_count
    bits = peers.bit_length() - 1
    orders = stage_orders(bits)
    streams = len(orders)
    outs = scatter_blocks(
        block_owner[:, 0],
        block_tile,
        block_count,
        obs_row,
        obs_col,
        offsets,
        obs_mask,
        innovations[0],
        orders,
        tile_local,
        cell_count,
    )
    keeps, sends = list(outs[:streams]), list(outs[streams:])
    for stage in range(bits):
        gots = [exchange(send, order[stage], peers) for send, order in zip(sends, orders)]
        sums = [added(kept, got) for kept, got in zip(keeps, gots)]
        if stage + 1 < bits:
            half = sums[0].shape[0] // 2
            sends = [total[half:].astype(jnp.bfloat16) for total in sums]
            keeps = [total[:half].astype(jnp.bfloat16) for total in sums]
    totals = jnp.concatenate(sums, axis=1)
    if ens_count > 1:
        totals = lax.psum(totals.astype(jnp.bfloat16), "ens").astype(jnp.float32)
    first = lax.axis_index("ens") * share
    return scaled_rows(totals, coupling, sigma, first, share, members)


def solution(mesh):
    in_specs = (
        P("ens", "space", None, None),
        P("space", None),
        P("space"),
        P("space"),
        P("space", None),
        P("space", None),
        P("space", None, None),
        P("space", None),
        P("space", None),
        P(),
    )
    out_specs = P("ens", "space", None)
    return jax.shard_map(
        on_device, mesh=mesh, in_specs=in_specs, out_specs=out_specs, check_vma=False
    )
```

```python
import functools

import jax
import jax.numpy as jnp
from jax import lax
from jax.experimental import pallas as pl
from jax.experimental.pallas import tpu as pltpu
from jax.sharding import PartitionSpec as P

TW = 16


def scaled_rows(totals, coupling, sigma, start, count, members):
    coupling_rows = lax.dynamic_slice_in_dim(coupling, start, count, 0)
    own = lax.dynamic_slice_in_dim(totals, start, count, 1)
    coupled = jnp.einsum("ck,tkh->cth", coupling_rows, totals, precision=lax.Precision.HIGHEST)
    return sigma[None, :, :] * (jnp.transpose(own, (1, 0, 2)) + coupled) / members


def stage_orders(bits):
    first = list(range(bits))
    second = list(first)
    if bits > 2:
        second[1], second[2] = second[2], second[1]
    return first, second


def scatter_kernel(
    head_ref,
    row_ref,
    col_ref,
    offsets_ref,
    mask_ref,
    values_ref,
    *refs,
    orders,
    tile_local,
    unroll,
    resumed,
):
    streams = len(orders)
    begun = refs[:streams] if resumed else ()
    refs = refs[len(begun) :]
    outs = refs[: streams * (2 if resumed else 1)]
    accs = refs[len(outs) : len(outs) + streams]
    lists = refs[len(outs) + streams :]
    blk_local, obs_count, width = values_ref.shape
    part = accs[0].shape[1]
    rows = streams * part // TW
    me = lax.axis_index("space")

    def pick(block, found):
        owner = head_ref[block]
        tile = head_ref[blk_local + block]
        relative = jnp.bitwise_xor(owner, me)
        lists[0][found] = block
        for order, slots in zip(orders, lists[1:]):
            place = jnp.int32(0)
            for bit in order[1:]:
                place = place * 2 + (lax.shift_right_logical(relative, bit) & 1)
            slots[found] = place * tile_local + tile
        return found + 1 - (lax.shift_right_logical(relative, orders[0][0]) & 1)

    count = jnp.minimum(head_ref[2 * blk_local], blk_local)
    found = lax.fori_loop(0, count, pick, jnp.int32(0))
    for step in range(unroll):
        for entries in lists:
            entries[found + step] = 0

    for index, acc in enumerate(accs):
        if resumed:
            acc[...] = begun[index][...].astype(jnp.float32)
        else:
            acc[...] = jnp.zeros(acc.shape, acc.dtype)
    row_ids = lax.broadcasted_iota(jnp.int32, (rows, obs_count), 0)
    col_ids = lax.broadcasted_iota(jnp.int32, (TW, obs_count), 0)

    def contribution(entry):
        block = lists[0][entry]
        row = row_ref[pl.ds(block, 1), :]
        col = col_ref[pl.ds(block, 1), :]
        row_frac = offsets_ref[block, 0:1, :]
        col_frac = offsets_ref[block, 1:2, :]
        alive = jnp.where(entry < found, 1.0, 0.0)
        live = mask_ref[pl.ds(block, 1), :].astype(jnp.float32) * alive
        row_off = row_ids - row
        row_part = jnp.where(
            row_off == 0,
            (1.0 - row_frac) * live,
            jnp.where(row_off == 1, row_frac * live, 0.0),
        )
        col_off = col_ids - col
        col_part = jnp.where(
            col_off == 0, 1.0 - col_frac, jnp.where(col_off == 1, col_frac, 0.0)
        )
        table = (row_part[:, None, :] * col_part[None, :, :]).reshape(rows * TW, obs_count)
        return jnp.dot(
            table.astype(jnp.bfloat16), values_ref[block], preferred_element_type=jnp.float32
        )

    def several(turn, carry):
        entries = [turn * unroll + step for step in range(unroll)]
        contribs = [contribution(entry) for entry in entries]
        for entry, contrib in zip(entries, contribs):
            for index, (slots, acc) in enumerate(zip(lists[1:], accs)):
                acc[slots[entry]] += contrib[index * part : (index + 1) * part]
        return carry

    lax.fori_loop(0, (found + unroll - 1) // unroll, several, 0)
    for index, acc in enumerate(accs):
        size = outs[0].shape[0]
        outs[index][...] = acc[:size].astype(outs[index].dtype)
        if resumed:
            outs[streams + index][...] = acc[size:].astype(outs[index].dtype)


def scatter_blocks(head, row, col, offsets, mask, values, begun, orders, tile_local, cells):
    streams = len(orders)
    slots = 2 ** (len(orders[0]) - 1) * tile_local
    part = cells // streams
    blk_local, _, width = values.shape
    unroll = 4
    resumed = bool(begun)
    out = jax.ShapeDtypeStruct((slots // 2 if resumed else slots, part, width), jnp.bfloat16)
    in_smem = pl.BlockSpec(memory_space=pltpu.SMEM)
    in_vmem = pl.BlockSpec(memory_space=pltpu.VMEM)
    outs = streams * (2 if resumed else 1)
    return pl.pallas_call(
        functools.partial(
            scatter_kernel, orders=orders, tile_local=tile_local, unroll=unroll, resumed=resumed
        ),
        in_specs=[in_smem] + [in_vmem] * (5 + len(begun)),
        out_specs=[in_vmem] * outs,
        out_shape=[out] * outs,
        scratch_shapes=[pltpu.VMEM((slots, part, width), jnp.float32)] * streams
        + [pltpu.SMEM((blk_local + unroll,), jnp.int32)] * (1 + streams),
    )(head, row, col, offsets, mask, values, *begun)


def exchange(part, bit, peers):
    return lax.ppermute(part, "space", [(i, i ^ (1 << bit)) for i in range(peers)])


def added(kept, got):
    return kept.astype(jnp.float32) + got.astype(jnp.float32)


def on_device(
    innovations,
    block_owner,
    block_tile,
    block_count,
    obs_row,
    obs_col,
    offsets,
    obs_mask,
    sigma,
    coupling,
):
    peers = lax.axis_size("space")
    tile_local = sigma.shape[0]
    cell_count = coupling.shape[0]
    ens_count = lax.axis_size("ens")
    members = ens_count * innovations.shape[0]
    share = cell_count // ens_count
    bits = peers.bit_length() - 1
    orders = stage_orders(bits)
    streams = len(orders)
    head = jnp.concatenate([block_owner[:, 0], block_tile, block_count])
    own = (head, obs_row, obs_col, offsets, obs_mask, innovations[0])
    other = tuple(exchange(array, orders[0][0], peers) for array in own)
    begun = scatter_blocks(*own, (), orders, tile_local, cell_count)
    outs = scatter_blocks(*other, begun, orders, tile_local, cell_count)
    keeps, sends = list(outs[:streams]), list(outs[streams:])
    for stage in range(1, bits):
        gots = [exchange(send, order[stage], peers) for send, order in zip(sends, orders)]
        sums = [added(kept, got) for kept, got in zip(keeps, gots)]
        if stage + 1 < bits:
            half = sums[0].shape[0] // 2
            sends = [total[half:].astype(jnp.bfloat16) for total in sums]
            keeps = [total[:half].astype(jnp.bfloat16) for total in sums]
    totals = jnp.concatenate(sums, axis=1)
    if ens_count > 1:
        totals = lax.psum(totals.astype(jnp.bfloat16), "ens").astype(jnp.float32)
    first = lax.axis_index("ens") * share
    return scaled_rows(totals, coupling, sigma, first, share, members)


def solution(mesh):
    in_specs = (
        P("ens", "space", None, None),
        P("space", None),
        P("space"),
        P("space"),
        P("space", None),
        P("space", None),
        P("space", None, None),
        P("space", None),
        P("space", None),
        P(),
    )
    out_specs = P("ens", "space", None)
    return jax.shard_map(
        on_device, mesh=mesh, in_specs=in_specs, out_specs=out_specs, check_vma=False
    )
```

```python
import functools

import jax
import jax.numpy as jnp
from jax import lax
from jax.experimental import pallas as pl
from jax.experimental.pallas import tpu as pltpu
from jax.sharding import PartitionSpec as P

TW = 16


def scaled_rows(totals, coupling, sigma, start, count, members):
    coupling_rows = lax.dynamic_slice_in_dim(coupling, start, count, 0)
    own = lax.dynamic_slice_in_dim(totals, start, count, 1)
    coupled = jnp.einsum("ck,tkh->cth", coupling_rows, totals, precision=lax.Precision.HIGHEST)
    return sigma[None, :, :] * (jnp.transpose(own, (1, 0, 2)) + coupled) / members


def stage_orders(bits):
    first = list(range(bits))
    second = list(first)
    if bits > 2:
        second[1], second[2] = second[2], second[1]
    return first, second


def scatter_kernel(
    owner_ref,
    tile_ref,
    count_ref,
    row_ref,
    col_ref,
    offsets_ref,
    mask_ref,
    values_ref,
    *refs,
    orders,
    tile_local,
    unroll,
):
    streams = len(orders)
    outs, accs = refs[: 2 * streams], refs[2 * streams : 3 * streams]
    staged = refs[3 * streams : 5 * streams]
    held_ref, in_sems, out_sems = refs[5 * streams :]
    blk_local, obs_count, width = values_ref.shape
    chunks = in_sems.shape[0]
    chunk = blk_local // chunks

    def load(index):
        rows_of = pl.ds(index * chunk, chunk)
        return pltpu.make_async_copy(
            values_ref.at[rows_of], held_ref.at[rows_of], in_sems.at[index]
        )

    for index in range(chunks):
        load(index).start()
    part = accs[0].shape[1]
    rows = streams * part // TW
    me = lax.axis_index("space")
    for acc in accs:
        acc[...] = jnp.zeros(acc.shape, acc.dtype)
    row_ids = lax.broadcasted_iota(jnp.int32, (rows, obs_count), 0)
    col_ids = lax.broadcasted_iota(jnp.int32, (TW, obs_count), 0)

    def one(block):
        relative = jnp.bitwise_xor(owner_ref[block], me)
        row = row_ref[pl.ds(block, 1), :]
        col = col_ref[pl.ds(block, 1), :]
        row_frac = offsets_ref[block, 0:1, :]
        col_frac = offsets_ref[block, 1:2, :]
        alive = jnp.where(block < count_ref[0], 1.0, 0.0)
        live = mask_ref[pl.ds(block, 1), :].astype(jnp.float32) * alive
        row_off = row_ids - row
        row_part = jnp.where(
            row_off == 0,
            (1.0 - row_frac) * live,
            jnp.where(row_off == 1, row_frac * live, 0.0),
        )
        col_off = col_ids - col
        col_part = jnp.where(
            col_off == 0, 1.0 - col_frac, jnp.where(col_off == 1, col_frac, 0.0)
        )
        table = (row_part[:, None, :] * col_part[None, :, :]).reshape(rows * TW, obs_count)
        contrib = jnp.dot(
            table.astype(jnp.bfloat16), held_ref[block], preferred_element_type=jnp.float32
        )
        for index, (order, acc) in enumerate(zip(orders, accs)):
            place = jnp.int32(0)
            for bit in order:
                place = place * 2 + (lax.shift_right_logical(relative, bit) & 1)
            slot = place * tile_local + tile_ref[block]
            acc[slot] += contrib[index * part : (index + 1) * part]

    def several(turn, carry):
        for step in range(unroll):
            one(turn * unroll + step)
        return carry

    for index in range(chunks):
        load(index).wait()
        first = index * chunk // unroll
        lax.fori_loop(first, first + chunk // unroll, several, 0)
    stores = []
    for side in (1, 0):
        for index, acc in enumerate(accs):
            at = side * streams + index
            half = staged[at].shape[0]
            staged[at][...] = acc[side * half : (side + 1) * half].astype(staged[at].dtype)
            store = pltpu.make_async_copy(staged[at], outs[at], out_sems.at[at])
            store.start()
            stores.append(store)
    for store in stores:
        store.wait()


def scatter_blocks(
    owner, block_tile, block_count, row, col, offsets, mask, values, orders, tile_local, cells
):
    streams = len(orders)
    slots = 2 ** len(orders[0]) * tile_local
    part = cells // streams
    width = values.shape[2]
    blk_local = values.shape[0]
    unroll, chunks = (4, 4) if blk_local % 16 == 0 else (1, 1)
    half = jax.ShapeDtypeStruct((slots // 2, part, width), jnp.bfloat16)
    in_smem = pl.BlockSpec(memory_space=pltpu.SMEM)
    in_vmem = pl.BlockSpec(memory_space=pltpu.VMEM)
    in_place = pl.BlockSpec(memory_space=pl.ANY)
    return pl.pallas_call(
        functools.partial(scatter_kernel, orders=orders, tile_local=tile_local, unroll=unroll),
        in_specs=[in_smem] * 3 + [in_vmem] * 4 + [in_place],
        out_specs=[in_place] * (2 * streams),
        out_shape=[half] * (2 * streams),
        scratch_shapes=[pltpu.VMEM((slots, part, width), jnp.float32)] * streams
        + [pltpu.VMEM(half.shape, half.dtype)] * (2 * streams)
        + [
            pltpu.VMEM(values.shape, values.dtype),
            pltpu.SemaphoreType.DMA((chunks,)),
            pltpu.SemaphoreType.DMA((2 * streams,)),
        ],
        compiler_params=pltpu.CompilerParams(vmem_limit_bytes=60 * 1024 * 1024),
    )(owner, block_tile, block_count, row, col, offsets, mask, values)


def exchange(part, mask, peers):
    return lax.ppermute(part, "space", [(i, i ^ mask) for i in range(peers)])


def added(kept, got):
    return kept.astype(jnp.float32) + got.astype(jnp.float32)


def on_device(
    innovations,
    block_owner,
    block_tile,
    block_count,
    obs_row,
    obs_col,
    offsets,
    obs_mask,
    sigma,
    coupling,
):
    peers = lax.axis_size("space")
    tile_local = sigma.shape[0]
    cell_count = coupling.shape[0]
    ens_count = lax.axis_size("ens")
    members = ens_count * innovations.shape[0]
    share = cell_count // ens_count
    bits = peers.bit_length() - 1
    orders = stage_orders(bits)
    streams = len(orders)
    outs = scatter_blocks(
        block_owner[:, 0],
        block_tile,
        block_count,
        obs_row,
        obs_col,
        offsets,
        obs_mask,
        innovations[0],
        orders,
        tile_local,
        cell_count,
    )
    keeps, sends = list(outs[:streams]), list(outs[streams:])
    for stage in range(bits - 2):
        gots = [exchange(send, 1 << order[stage], peers) for send, order in zip(sends, orders)]
        sums = [added(kept, got).astype(jnp.bfloat16) for kept, got in zip(keeps, gots)]
        half = sums[0].shape[0] // 2
        sends = [total[half:] for total in sums]
        keeps = [total[:half] for total in sums]
    joined = jnp.concatenate(sums, axis=1)
    quarters = [joined[i * tile_local : (i + 1) * tile_local] for i in range(4)]
    high, low = 1 << orders[0][-2], 1 << orders[0][-1]
    gots = [
        exchange(quarters[3], high | low, peers),
        exchange(quarters[2], high, peers),
        exchange(quarters[1], low, peers),
    ]
    totals = quarters[0].astype(jnp.float32)
    for got in gots:
        totals = totals + got.astype(jnp.float32)
    if ens_count > 1:
        totals = lax.psum(totals.astype(jnp.bfloat16), "ens").astype(jnp.float32)
    first = lax.axis_index("ens") * share
    return scaled_rows(totals, coupling, sigma, first, share, members)


def solution(mesh):
    in_specs = (
        P("ens", "space", None, None),
        P("space", None),
        P("space"),
        P("space"),
        P("space", None),
        P("space", None),
        P("space", None, None),
        P("space", None),
        P("space", None),
        P(),
    )
    out_specs = P("ens", "space", None)
    return jax.shard_map(
        on_device, mesh=mesh, in_specs=in_specs, out_specs=out_specs, check_vma=False
    )
```
